32 devices in a mesh: rep: 1 (over z), dp: 32 (over x, y, core).
Axes of the slice: x: 4, y: 4, z: 1, core: 2. Of those that a mesh axis runs over, the one named last changes fastest.
The devices are a block of a 4x4x8 slice.
Arguments:
- x: bfloat16 [32, 2048, 1024], P(('rep', 'dp'))
- dy: bfloat16 [32, 2048, 1024], P(('rep', 'dp'))
- w_gate: bfloat16 [2, 1024, 3200], P(None, 'dp')
- w_up: bfloat16 [2, 1024, 3200], P(None, 'dp')
- w_down: bfloat16 [2, 3200, 1024], P(None, 'dp')
Outputs:
- output 1: bfloat16 [32, 2048, 1024], P(('rep', 'dp'))
- output 2: bfloat16 [2, 1024, 3200], P('rep', 'dp')
- output 3: bfloat16 [2, 1024, 3200], P('rep', 'dp')
- output 4: bfloat16 [2, 3200, 1024], P('rep', 'dp')
All inputs are finite; a program needn't handle non-finite values.
Results may differ from the reference program's by a relative error of at most 0.018.
Values are sent between devices in bfloat16 or wider.
A program may use at most 768 MiB of HBM per device.

```python
import jax
import jax.numpy as jnp
from jax import lax

SEQUENCES = 32
TOKENS = 2048
D = 1024
FF = 3200
LAYERS = 2
NAMES = ("w_gate", "w_up", "w_down")
SHAPES = {"w_gate": (LAYERS, D, FF), "w_up": (LAYERS, D, FF), "w_down": (LAYERS, FF, D)}


def bump(key, n, height):
    away = (jnp.arange(n, dtype=jnp.int32) - jax.random.randint(key, (), 0, n, jnp.int32)) % n
    return jnp.where(away < n // 8, height, 1.0)


def together(key, own, strength):
    shared = jax.random.normal(key, own.shape[1:], jnp.float32)
    return (own + strength * shared) * lax.rsqrt(1 + strength * strength)


def setup_inputs(seed: int = 0, part: int = 0) -> dict:
    kx, kdy, ka, kb, kz, kf, kh, kl, *kw = jax.random.split(jax.random.key(seed), 8 + len(NAMES))
    kx, kdy, ka, kb = (jax.random.fold_in(k, part) for k in (kx, kdy, ka, kb))
    shape = (SEQUENCES, TOKENS, D)
    much_x, much_dy = jax.random.uniform(kz, (2,), jnp.float32, 0.0, 1.0)
    layers = 2.0 ** jax.random.uniform(kl, (LAYERS, 1, 1), jnp.float32, -1.0, 1.0)
    x = together(ka, jax.random.normal(kx, shape, jnp.float32), much_x) * bump(kf, D, 4.0)
    dy = together(kb, jax.random.normal(kdy, shape, jnp.float32), much_dy)
    drawn = {"x": x.astype(jnp.bfloat16), "dy": (dy * (SEQUENCES * TOKENS) ** -0.5).astype(jnp.bfloat16)}
    for key, name in zip(kw, NAMES, strict=True):
        w = jax.random.normal(key, SHAPES[name], jnp.float32) * SHAPES[name][1] ** -0.5
        drawn[name] = (w * {"w_gate": 1.0, "w_up": bump(kh, FF, 4.0), "w_down": layers}[name]).astype(jnp.bfloat16)
    return drawn


def matmul(a, w):
    return jnp.dot(a, w, preferred_element_type=jnp.float32).astype(jnp.bfloat16)


def normed(h):
    wide = h.astype(jnp.float32)
    scale = lax.rsqrt(jnp.mean(wide**2, -1, keepdims=True) + 1e-6)
    return (wide * scale).astype(jnp.bfloat16)


def layer(h, w):
    a = normed(h)
    gate = jnp.dot(a, w["w_gate"], preferred_element_type=jnp.float32)
    up = jnp.dot(a, w["w_up"], preferred_element_type=jnp.float32)
    return h + matmul((jax.nn.silu(gate) * up).astype(jnp.bfloat16), w["w_down"])


def stack(weights, h):
    return lax.scan(lambda h, w: (layer(h, w), None), h, weights)[0]


def reference(x, dy, w_gate, w_up, w_down):
    weights = dict(zip(NAMES, (w_gate, w_up, w_down), strict=True))

    def take(so_far, sequence):
        h, by_y = sequence
        _, back = jax.vjp(stack, weights, h)
        by_weights, by_h = back(by_y)
        return jax.tree.map(lambda total, term: total + term.astype(jnp.float32), so_far, by_weights), by_h

    none_yet = {name: jnp.zeros(w.shape, jnp.float32) for name, w in weights.items()}
    by_weights, by_x = lax.scan(take, none_yet, (x, dy))
    return (by_x, *(by_weights[name].astype(jnp.bfloat16) for name in NAMES))
```

```python
import functools
import math

import jax
import jax.numpy as jnp
from jax import lax
from jax.experimental import pallas as pl
from jax.experimental.pallas import tpu as pltpu
from jax.sharding import PartitionSpec as P

F32, BF16 = jnp.float32, jnp.bfloat16
MESH = pl.DeviceIdType.MESH
ALL = slice(None)
RING = 4
EPS = 1e-6
BM = 256
VMEM_LIMIT = 66_000_000


class Place:
    def __init__(self):
        me = lax.axis_index("dp")
        self.core = lax.rem(me, 2)
        chip = me // 2
        self.y = lax.rem(chip, RING)
        self.x = chip // RING

    def device(self, colour, p, q, core=None):
        x, y = (p, q) if colour == 0 else (q, p)
        return {"dp": (x * RING + y) * 2 + (self.core if core is None else core)}

    def peer(self):
        return self.device(0, self.x, self.y, 1 - self.core)

    def pq(self, colour):
        return (self.x, self.y) if colour == 0 else (self.y, self.x)


def ahead(i, by):
    return lax.rem(i + by, RING)


def greet():
    here = Place()
    barrier = pltpu.get_barrier_semaphore()
    (x, y) = here.x, here.y
    others = [here.peer()]
    for by in (1, RING - 1):
        others += [here.device(0, ahead(x, by), y), here.device(0, x, ahead(y, by))]
    for other in others:
        pl.semaphore_signal(barrier, inc=1, device_id=other, device_id_type=MESH)
    pl.semaphore_wait(barrier, len(others))


class Piece:
    def __init__(self, kind, rows, columns):
        self.kind, self.rows, self.columns = kind, rows, columns

    def sub(self, colour, half):
        if self.kind == "row":
            r = (self.rows // 2 * colour, self.rows // 2)
            first = (self.columns // 128 + 1) // 2 * 128
            c = {None: (0, self.columns), 0: (0, first), 1: (first, self.columns - first)}[half]
        else:
            r = (0, self.rows)
            wide = self.columns // 2
            c = {None: (0, wide), 0: (0, wide // 2), 1: (wide // 2, wide // 2)}[half]
            c = (c[0] + wide * colour, c[1])
        return r, c

    def shape(self, colour, half):
        r, c = self.sub(colour, half)
        return (r[1], c[1])

    def inside(self, half):
        r, c = self.sub(0, half)
        return pl.ds(c[0], c[1])

    def of_whole(self, ref, core, colour, p, q, half=None):
        x, y = (p, q) if colour == 0 else (q, p)
        r, c = self.sub(colour, half)
        if self.kind == "row":
            return ref.at[x, y, core, pl.ds(*r), pl.ds(*c)]
        return ref.at[x, y, pl.ds(*r), pl.ds(pl.multiple_of(core * self.columns + c[0], 128), c[1])]

    def all_of_core(self, ref, core):
        if self.kind == "row":
            return ref.at[:, :, core]
        return ref.at[:, :, :, pl.ds(pl.multiple_of(core * self.columns, 128), self.columns)]

    def chip_of_core(self, ref, core, x, y):
        if self.kind == "row":
            return ref.at[x, y, core]
        return ref.at[x, y, :, pl.ds(pl.multiple_of(core * self.columns, 128), self.columns)]

    def of_own(self, ref, colour, half=None):
        r, c = self.sub(colour, half)
        return ref.at[pl.ds(*r), pl.ds(*c)]

    def of_pieces(self, ref, colour, p, q, half=None):
        x, y = (p, q) if colour == 0 else (q, p)
        r, c = self.sub(colour, half)
        return ref.at[x, y, pl.ds(*r), pl.ds(*c)]

    def whole_shape(self):
        if self.kind == "row":
            return (RING, RING, 2, self.rows, self.columns)
        return (RING, RING, self.rows, 2 * self.columns)


def remote(src, dst, sems, k, device):
    send, recv = sems
    return pltpu.make_async_remote_copy(
        src_ref=src, dst_ref=dst, send_sem=send.at[k], recv_sem=recv.at[k], device_id=device, device_id_type=MESH
    )


class Gather:
    N = 24

    def __init__(self, piece):
        self.piece = piece

    def scratch(self):
        return [pltpu.SemaphoreType.DMA((self.N,)), pltpu.SemaphoreType.DMA((self.N,)), pltpu.SemaphoreType.DMA]

    def bind(self, own, whole, send, recv, local):
        self.own, self.whole, self.sems, self.local = own, whole, (send, recv), local
        return self

    def copies(self, here):
        piece, own, whole, core = self.piece, self.own, self.whole, here.core
        out = {}

        def of_colour(colour):
            p, q = here.pq(colour)
            p1, pm, q1, qm = ahead(p, 1), ahead(p, RING - 1), ahead(q, 1), ahead(q, RING - 1)
            q2 = ahead(q, 2)
            at = functools.partial(piece.of_whole, whole, core, colour)
            dev = functools.partial(here.device, colour)
            base = 12 * colour

            def add(name, k, src, dst, device):
                out[name, colour] = lambda: remote(src(), dst(), self.sems, base + k, device)

            mine = lambda: piece.of_own(own, colour)
            add("s1+", 0, mine, lambda: at(p, q), dev(p1, q))
            add("s1-", 1, mine, lambda: at(p, q), dev(pm, q))
            add("s2+", 2, lambda: at(pm, q, 0), lambda: at(pm, q, 0), dev(p1, q))
            add("s2-", 3, lambda: at(p1, q, 1), lambda: at(p1, q, 1), dev(pm, q))
            add("s3+", 4, lambda: at(ALL, q), lambda: at(ALL, q), dev(p, q1))
            add("s3-", 5, lambda: at(ALL, q), lambda: at(ALL, q), dev(p, qm))
            add("s4+", 6, lambda: at(ALL, qm, 0), lambda: at(ALL, qm, 0), dev(p, q1))
            add("s4-", 7, lambda: at(ALL, q1, 1), lambda: at(ALL, q1, 1), dev(p, qm))
            for k, of in ((8, q), (9, qm), (10, q1), (11, q2)):
                add(f"d{k}", k, lambda of=of: at(ALL, of), lambda of=of: at(ALL, of), here.peer())

        of_colour(0)
        of_colour(1)
        return out

    def run(self, stage):
        here = Place()
        c = self.copies(here)
        both = lambda names, do: [do(c[name, colour]()) for name in names for colour in (0, 1)]
        start = lambda *names: both(names, lambda d: d.start())
        arrived = lambda *names: both(names, lambda d: d.wait_recv())
        local = lambda: pltpu.make_async_copy(
            self.own, self.piece.chip_of_core(self.whole, here.core, here.x, here.y), self.local
        )
        if stage == 0:
            start("s1+", "s1-")
            local().start()
        elif stage == 1:
            for name, then in (("s1+", "s2+"), ("s1-", "s2-")):
                arrived(name)
                start(then)
        elif stage == 2:
            local().wait()
            arrived("s2+", "s2-")
            start("s3+", "s3-", "d8")
        elif stage == 3:
            for name, then, peer in (("s3+", "s4+", "d9"), ("s3-", "s4-", "d10")):
                arrived(name)
                start(then, peer)
        elif stage == 4:
            arrived("s4+", "s4-")
            start("d11")
        else:
            arrived("d8", "d9", "d10", "d11")
            both([n for n, colour in c if colour == 0], lambda d: d.wait_send())

    STAGES = 6


class Scatter:
    STAGES = 6

    def __init__(self, piece):
        self.piece = piece

    def scratch(self):
        piece = self.piece
        full = (RING, RING, piece.rows, piece.columns)
        c, h0, h1 = piece.shape(0, None), piece.shape(0, 0), piece.shape(0, 1)
        vm = lambda *shape, dtype=BF16: pltpu.VMEM(shape, dtype)
        per = [
            vm(2, RING, *h0), vm(2, RING, *h1), vm(2, RING, *c), vm(2, RING, *c),
            vm(2, *h0), vm(2, *h1), vm(2, *c), vm(2, *c),
            vm(2, RING, *c, dtype=F32),
        ]
        return [
            vm(*full), vm(*full), *per,
            pltpu.SemaphoreType.DMA((17,)), pltpu.SemaphoreType.DMA((17,)), pltpu.SemaphoreType.DMA,
        ]

    def bind(self, terms, result, *scratch):
        self.terms, self.result = terms, result
        self.t, self.r, *self.landing, self.acc, send, recv, self.local = scratch
        self.sems = (send, recv)
        return self

    def copies(self, here):
        piece, t = self.piece, self.t
        far_a, far_b, near_a, near_b, last_far_a, last_far_b, last_near_a, last_near_b = self.landing
        out = {}

        def of_colour(colour):
            p, q = here.pq(colour)
            p1, pm, p2 = ahead(p, 1), ahead(p, RING - 1), ahead(p, 2)
            q1, qm, q2 = ahead(q, 1), ahead(q, RING - 1), ahead(q, 2)
            at = functools.partial(piece.of_pieces, t, colour)
            dev = functools.partial(here.device, colour)
            base = 8 * colour

            def add(name, k, src, dst, device):
                out[name, colour] = lambda: remote(src(), dst.at[colour], self.sems, base + k, device)

            add("F+", 0, lambda: at(ALL, q2, 0), far_a, dev(p, q1))
            add("F-", 1, lambda: at(ALL, q2, 1), far_b, dev(p, qm))
            add("N+", 2, lambda: at(ALL, q1), near_a, dev(p, q1))
            add("N-", 3, lambda: at(ALL, qm), near_b, dev(p, qm))
            add("f+", 4, lambda: at(p2, q, 0), last_far_a, dev(p1, q))
            add("f-", 5, lambda: at(p2, q, 1), last_far_b, dev(pm, q))
            add("n+", 6, lambda: at(p1, q), last_near_a, dev(p1, q))
            add("n-", 7, lambda: at(pm, q), last_near_b, dev(pm, q))

        of_colour(0)
        of_colour(1)
        return out

    def run(self, stage):
        here = Place()
        piece, t, r, acc = self.piece, self.t, self.r, self.acc
        far_a, far_b, near_a, near_b, last_far_a, last_far_b, last_near_a, last_near_b = self.landing
        c = self.copies(here)
        both = lambda names, do: [do(c[name, colour]()) for name in names for colour in (0, 1)]
        arrived = lambda *names: both(names, lambda d: d.wait_recv())
        peer = lambda: remote(piece.all_of_core(self.terms, 1 - here.core), r, self.sems, 16, here.peer())
        local = lambda: pltpu.make_async_copy(piece.all_of_core(self.terms, here.core), t, self.local)
        wide = lambda ref: ref[...].astype(F32)
        if stage == 0:
            peer().start()
            local().start()
            return
        if stage == 1:
            local().wait()
            peer().wait_recv()
        if stage == 2:
            arrived("F+", "F-")
        if stage == 3:
            arrived("N+", "N-")
        if stage == 4:
            arrived("f+", "f-")
        if stage == 5:
            arrived("n+", "n-")
        for colour in (0, 1):
            p, q = here.pq(colour)
            p1, pm, p2 = ahead(p, 1), ahead(p, RING - 1), ahead(p, 2)
            q1, qm, q2 = ahead(q, 1), ahead(q, RING - 1), ahead(q, 2)
            own = lambda pp, qq, half=None: wide(piece.of_pieces(t, colour, pp, qq, half)) + wide(
                piece.of_pieces(r, colour, pp, qq, half)
            )

            def put(pp, qq, value, half=None):
                piece.of_pieces(t, colour, pp, qq, half)[...] = value.astype(BF16)

            h0, h1 = piece.inside(0), piece.inside(1)
            if stage == 1:
                for i in range(RING):
                    put(i, q2, own(i, q2))
                c["F+", colour]().start()
                c["F-", colour]().start()
            elif stage == 2:
                for i in range(RING):
                    put(i, q1, own(i, q1, 0) + far_a[colour, i].astype(F32), 0)
                    put(i, q1, own(i, q1, 1), 1)
                c["N+", colour]().start()
                for i in range(RING):
                    put(i, qm, own(i, qm, 0), 0)
                    put(i, qm, own(i, qm, 1) + far_b[colour, i].astype(F32), 1)
                c["N-", colour]().start()
            elif stage == 3:
                for i in range(RING):
                    acc[colour, i] = own(i, q) + near_a[colour, i].astype(F32) + near_b[colour, i].astype(F32)
                put(p2, q, acc[colour, p2])
                c["f+", colour]().start()
                c["f-", colour]().start()
            elif stage == 4:
                put(p1, q, acc[colour, p1, :, h0] + last_far_a[colour].astype(F32), 0)
                put(p1, q, acc[colour, p1, :, h1], 1)
                c["n+", colour]().start()
                put(pm, q, acc[colour, pm, :, h0], 0)
                put(pm, q, acc[colour, pm, :, h1] + last_far_b[colour].astype(F32), 1)
                c["n-", colour]().start()
            else:
                total = acc[colour, p] + last_near_a[colour].astype(F32) + last_near_b[colour].astype(F32)
                piece.of_own(self.result, colour)[...] = total.astype(BF16)
        if stage == 5:
            peer().wait_send()
            both([n for n, colour in c if colour == 0], lambda d: d.wait_send())


def kernel_call(name, grid, compute, inputs, outputs, parts=1, gathers=(), scatters=(), at=None, collective_id=None, scratch=()):
    comms = [Gather(p) for p, _ in gathers] + [Scatter(p) for p, _ in scatters]
    n_in, n_out = len(inputs), len(outputs)
    steps = math.prod(grid)
    any_space = pl.BlockSpec(memory_space=pltpu.HBM)
    in_vmem = lambda shape: pl.BlockSpec(shape, lambda *_: (0,) * len(shape), pipeline_mode=pl.Buffered(1))

    def spec(block, index):
        if index is None:
            return in_vmem(block)
        return pl.BlockSpec(block, index)

    in_specs = [spec(b, i) for _, b, i in inputs]
    out_specs = [spec(b, i) for *_, b, i in outputs]
    out_shape = [jax.ShapeDtypeStruct(s, d) for s, d, *_ in outputs]
    args = [a for a, *_ in inputs]
    for piece, own in gathers:
        args.append(own)
        in_specs.append(in_vmem(own.shape))
        out_shape.append(jax.ShapeDtypeStruct(piece.whole_shape(), BF16))
        out_specs.append(any_space)
    for piece, terms in scatters:
        args.append(terms)
        in_specs.append(any_space)
        shape = (piece.rows, piece.columns)
        out_shape.append(jax.ShapeDtypeStruct(shape, BF16))
        out_specs.append(in_vmem(shape))
    comm_scratch = [c.scratch() for c in comms]
    scratch_shapes = [*scratch, *(s for group in comm_scratch for s in group)]
    last = steps * parts
    if comms and at is None:
        at = [min(last, k * last // 6) for k in range(6)]

    def body(*refs):
        refs = list(refs)
        take = lambda n: [refs.pop(0) for _ in range(n)]
        ins, comm_in = take(n_in), take(len(comms))
        outs, comm_out = take(n_out), take(len(comms))
        own_scratch = take(len(scratch))
        for comm, i, o, s in zip(comms, comm_in, comm_out, comm_scratch):
            comm.bind(i, o, *take(len(s)))
        step = pl.program_id(0)
        for d in range(1, len(grid)):
            step = step * grid[d] + pl.program_id(d)

        def act(slot):
            if slot == 0:
                greet()
            for k in range(6):
                if at[k] == slot:
                    for comm in comms:
                        comm.run(k)

        def hook(part):
            if not comms:
                return
            for slot in sorted({0, *at}):
                if slot < last and slot % parts == part:
                    pl.when(step == slot // parts)(functools.partial(act, slot))

        compute(hook, step, ins, outs, own_scratch)
        if comms and any(a == last for a in at):
            pl.when(step == steps - 1)(functools.partial(act, last))

    params = dict(vmem_limit_bytes=VMEM_LIMIT, dimension_semantics=("arbitrary",) * len(grid))
    if comms:
        params |= dict(collective_id=collective_id, has_side_effects=True)
    return pl.pallas_call(
        body, grid=grid, in_specs=in_specs, out_specs=out_specs, out_shape=out_shape, scratch_shapes=scratch_shapes,
        compiler_params=pltpu.CompilerParams(**params), name=name,
    )(*args)


def dot(a, b, ca=1, cb=0):
    return lax.dot_general(a, b, (((ca,), (cb,)), ((), ())), preferred_element_type=F32)


def chunks(n, size=512):
    return [(i, min(size, n - i)) for i in range(0, n, size)]


def normed(h):
    wide = h.astype(F32)
    scale = lax.rsqrt(jnp.mean(wide**2, -1, keepdims=True) + EPS)
    return (wide * scale).astype(BF16)


def norm_back(h, da, dy):
    wide, da = h.astype(F32), da.astype(F32)
    scale = lax.rsqrt(jnp.mean(wide**2, -1, keepdims=True) + EPS)
    by_scale = jnp.sum(da * wide, -1, keepdims=True)
    by_mean = by_scale * (-0.5) * scale * scale * scale
    return dy + (da * scale + wide * (by_mean * (2.0 / h.shape[-1]))).astype(BF16)


def gated(g, u):
    s = jax.nn.sigmoid(g)
    return (g * s * u).astype(BF16)


def gated_back(g, u, dh):
    s = jax.nn.sigmoid(g)
    silu = g * s
    return ((dh * u) * (s + silu * (1.0 - s))).astype(BF16), (dh * silu).astype(BF16)


def rows_of(array, bm=BM):
    block = (bm, *array.shape[1:])
    return array, block, lambda i: (i, 0)


def whole(array):
    return array, array.shape, None


def k_norm(x, **comm):
    t, d = x.shape

    def compute(hook, step, ins, outs, _):
        hook(0)
        outs[0][...] = normed(ins[0][...])

    bm = t // 8
    return kernel_call("norm", (8,), compute, [rows_of(x, bm)], [((t, d), BF16, (bm, d), lambda i: (i, 0))], **comm)


def k_gate_up(a, wg, wu, **comm):
    t, f = a.shape[0], wg.shape[1]

    def compute(hook, step, ins, outs, _):
        a, wg, wu = ins
        g_out, u_out, h_out = outs
        x = a[...]
        hook(0)
        for lo, n in chunks(f):
            cols = pl.ds(lo, n)
            g, u = dot(x, wg[:, cols]), dot(x, wu[:, cols])
            g_out[:, cols] = g
            u_out[:, cols] = u
            h_out[:, cols] = gated(g, u)

    o = lambda dt: ((t, f), dt, (BM, f), lambda i: (i, 0))
    return kernel_call("gate_up", (t // BM,), compute, [rows_of(a), whole(wg), whole(wu)], [o(F32), o(F32), o(BF16)], **comm)


def k_down(h, x, wd, **comm):
    t, d = x.shape

    def compute(hook, step, ins, outs, _):
        h, x, wd = ins
        hook(0)
        y = x[...] + dot(h[...], wd[...]).astype(BF16)
        outs[0][...] = y
        outs[1][...] = normed(y)

    o = ((t, d), BF16, (BM, d), lambda i: (i, 0))
    return kernel_call("down", (t // BM,), compute, [rows_of(h), rows_of(x), whole(wd)], [o, o], **comm)


def k_middle(a, dy, wg, wu, wd):
    t, f = a.shape[0], wg.shape[1]

    def compute(hook, step, ins, outs, _):
        a, dy, wg, wu, wd = ins
        dgu, h_out = outs
        x, dy = a[...], dy[...]
        for lo, n in chunks(f):
            cols = pl.ds(lo, n)
            g, u = dot(x, wg[:, cols]), dot(x, wu[:, cols])
            dh = dot(dy, wd[cols, :], 1, 1).astype(BF16).astype(F32)
            h_out[:, cols] = gated(g, u)
            dgu[0, :, cols], dgu[1, :, cols] = gated_back(g, u, dh)

    return kernel_call(
        "middle", (t // BM,), compute,
        [rows_of(a), rows_of(dy), whole(wg), whole(wu), whole(wd)],
        [((2, t, f), BF16, (2, BM, f), lambda i: (0, i, 0)), ((t, f), BF16, (BM, f), lambda i: (i, 0))],
    )


def k_hidden_back(dy, g, u, wd, **comm):
    t, f = g.shape

    def compute(hook, step, ins, outs, _):
        dy, g, u, wd = ins
        (dgu,) = outs
        hook(0)
        x = dy[...]
        for lo, n in chunks(f):
            cols = pl.ds(lo, n)
            dh = dot(x, wd[cols, :], 1, 1).astype(BF16).astype(F32)
            dgu[0, :, cols], dgu[1, :, cols] = gated_back(g[:, cols], u[:, cols], dh)

    return kernel_call(
        "hidden_back", (t // BM,), compute, [rows_of(dy), rows_of(g), rows_of(u), whole(wd)],
        [((2, t, f), BF16, (2, BM, f), lambda i: (0, i, 0))], **comm,
    )


def k_grad_down(h, dy, **comm):
    (t, f), d = h.shape, dy.shape[1]
    bn = f // 5

    def compute(hook, step, ins, outs, _):
        hook(0)
        outs[0][...] = dot(ins[0][...], ins[1][...], 0, 0).astype(BF16)

    return kernel_call(
        "grad_down", (5,), compute, [(h, (t, bn), lambda i: (0, i)), whole(dy)],
        [((f, d), BF16, (bn, d), lambda i: (i, 0))], **comm,
    )


def k_grad_gate_up(a, dgu, **comm):
    (t, d), f = a.shape, dgu.shape[2]
    bm = d // 4

    def compute(hook, step, ins, outs, _):
        a, dgu = ins
        x = a[...]
        hook(0)
        for lo, n in chunks(f):
            cols = pl.ds(lo, n)
            outs[0][0, :, cols] = dot(x, dgu[0, :, cols], 0, 0).astype(BF16)

    return kernel_call(
        "grad_gate_up", (2, 4), compute,
        [(a, (t, bm), lambda w, i: (0, i)), (dgu, (1, t, f), lambda w, i: (w, 0, 0))],
        [((2, d, f), BF16, (1, bm, f), lambda w, i: (w, i, 0))], **comm,
    )


def k_input_back(dgu, wg, wu, x, dy, **comm):
    t, d = x.shape
    f = dgu.shape[2]

    def compute(hook, step, ins, outs, _):
        dgu, wg, wu, x, dy = ins
        hook(0)
        da = dot(dgu[0], wg[...], 1, 1).astype(BF16) + dot(dgu[1], wu[...], 1, 1).astype(BF16)
        outs[0][...] = norm_back(x[...], da, dy[...])

    return kernel_call(
        "input_back", (t // BM,), compute,
        [(dgu, (2, BM, f), lambda i: (0, i, 0)), whole(wg), whole(wu), rows_of(x), rows_of(dy)],
        [((t, d), BF16, (BM, d), lambda i: (i, 0))], **comm,
    )


def solution(mesh):
    members = mesh.shape["dp"]
    swap = [(i, i ^ 1) for i in range(members)]

    def step(x, dy, w_gate, w_up, w_down):
        x, dy = x[0], dy[0]
        core = lax.rem(lax.axis_index("dp"), 2)
        rows, f = w_gate.shape[1:]
        deep, d = w_down.shape[1:]
        half = d // 2
        row, col = Piece("row", rows, f), Piece("col", 2 * deep, half)
        square = lambda w: w.reshape(-1, w.shape[-1])

        keep = lax.dynamic_slice_in_dim(w_down, core * half, half, 2)
        other = lax.ppermute(lax.dynamic_slice_in_dim(w_down, (1 - core) * half, half, 2), "dp", swap)
        down = jnp.where(core == 0, jnp.concatenate([keep, other], 1), jnp.concatenate([other, keep], 1))

        a0, wg0, wu0 = k_norm(x, gathers=[(row, w_gate[0]), (row, w_up[0])], collective_id=0)
        wg0, wu0 = square(wg0), square(wu0)
        g0, u0, h0, wd0, wg1 = k_gate_up(a0, wg0, wu0, gathers=[(col, down[0]), (row, w_gate[1])], collective_id=1)
        wd0, wg1 = square(wd0), square(wg1)
        x1, a1, wu1, wd1 = k_down(h0, x, wd0, gathers=[(row, w_up[1]), (col, down[1])], collective_id=2)
        wu1, wd1 = square(wu1), square(wd1)

        as_row = lambda g: g.reshape(RING, RING, 2, rows, f)
        as_col = lambda g: g.reshape(RING, RING, 2 * deep, d)
        dgu1, h1 = k_middle(a1, dy, wg1, wu1, wd1)
        (gd1,) = k_grad_down(h1, dy)
        ggu1, by_d1 = k_grad_gate_up(a1, dgu1, scatters=[(col, as_col(gd1))], collective_id=3)
        dx1, by_g1 = k_input_back(dgu1, wg1, wu1, x1, dy, scatters=[(row, as_row(ggu1[0]))], collective_id=4)
        dgu0, by_u1 = k_hidden_back(dx1, g0, u0, wd0, scatters=[(row, as_row(ggu1[1]))], collective_id=5)
        (gd0,) = k_grad_down(h0, dx1)
        ggu0, by_d0 = k_grad_gate_up(a0, dgu0, scatters=[(col, as_col(gd0))], collective_id=6)
        by_x, by_g0, by_u0 = k_input_back(
            dgu0, wg0, wu0, x, dx1, scatters=[(row, as_row(ggu0[0])), (row, as_row(ggu0[1]))], collective_id=7
        )

        by_down = jnp.stack([by_d0, by_d1])
        mine = lax.dynamic_slice_in_dim(by_down, core * deep, deep, 1)
        theirs = lax.ppermute(lax.dynamic_slice_in_dim(by_down, (1 - core) * deep, deep, 1), "dp", swap)
        by_down = jnp.where(core == 0, jnp.concatenate([mine, theirs], 2), jnp.concatenate([theirs, mine], 2))
        return by_x[None], jnp.stack([by_g0, by_g1]), jnp.stack([by_u0, by_u1]), by_down

    tokens, weights, grads = P(("rep", "dp")), P(None, "dp"), P("rep", "dp")
    return jax.shard_map(
        step, mesh=mesh, in_specs=(tokens, tokens, weights, weights, weights), out_specs=(tokens, grads, grads, grads),
        check_vma=False,
    )
```

```python
import functools
import math

import jax
import jax.numpy as jnp
from jax import lax
from jax.experimental import pallas as pl
from jax.experimental.pallas import tpu as pltpu
from jax.sharding import PartitionSpec as P

F32, BF16 = jnp.float32, jnp.bfloat16
MESH = pl.DeviceIdType.MESH
ALL = slice(None)
RING = 4
EPS = 1e-6
BM = 256
CHUNK = 1024
GRAD_ROWS = 256
VMEM_LIMIT = 66_000_000


class Place:
    def __init__(self):
        me = lax.axis_index("dp")
        self.core = lax.rem(me, 2)
        chip = me // 2
        self.y = lax.rem(chip, RING)
        self.x = chip // RING

    def device(self, colour, p, q, core=None):
        x, y = (p, q) if colour == 0 else (q, p)
        return {"dp": (x * RING + y) * 2 + (self.core if core is None else core)}

    def peer(self):
        return self.device(0, self.x, self.y, 1 - self.core)

    def pq(self, colour):
        return (self.x, self.y) if colour == 0 else (self.y, self.x)


def ahead(i, by):
    return lax.rem(i + by, RING)


def greet():
    here = Place()
    barrier = pltpu.get_barrier_semaphore()
    (x, y) = here.x, here.y
    others = [here.peer()]
    for by in (1, RING - 1):
        others += [here.device(0, ahead(x, by), y), here.device(0, x, ahead(y, by))]
    for other in others:
        pl.semaphore_signal(barrier, inc=1, device_id=other, device_id_type=MESH)
    pl.semaphore_wait(barrier, len(others))


class Piece:
    def __init__(self, kind, rows, columns):
        self.kind, self.rows, self.columns = kind, rows, columns

    def sub(self, colour, half):
        if self.kind == "row":
            r = (self.rows // 2 * colour, self.rows // 2)
            first = (self.columns // 128 + 1) // 2 * 128
            c = {None: (0, self.columns), 0: (0, first), 1: (first, self.columns - first)}[half]
        else:
            r = (0, self.rows)
            wide = self.columns // 2
            c = {None: (0, wide), 0: (0, wide // 2), 1: (wide // 2, wide // 2)}[half]
            c = (c[0] + wide * colour, c[1])
        return r, c

    def shape(self, colour, half):
        r, c = self.sub(colour, half)
        return (r[1], c[1])

    def inside(self, half):
        r, c = self.sub(0, half)
        return pl.ds(c[0], c[1])

    def of_whole(self, ref, core, colour, p, q, half=None):
        x, y = (p, q) if colour == 0 else (q, p)
        r, c = self.sub(colour, half)
        if self.kind == "row":
            return ref.at[x, y, core, pl.ds(*r), pl.ds(*c)]
        return ref.at[x, y, pl.ds(*r), pl.ds(pl.multiple_of(core * self.columns + c[0], 128), c[1])]

    def all_of_core(self, ref, core):
        if self.kind == "row":
            return ref.at[:, :, core]
        return ref.at[:, :, :, pl.ds(pl.multiple_of(core * self.columns, 128), self.columns)]

    def chip_of_core(self, ref, core, x, y):
        if self.kind == "row":
            return ref.at[x, y, core]
        return ref.at[x, y, :, pl.ds(pl.multiple_of(core * self.columns, 128), self.columns)]

    def of_own(self, ref, colour, half=None):
        r, c = self.sub(colour, half)
        return ref.at[pl.ds(*r), pl.ds(*c)]

    def of_pieces(self, ref, colour, p, q, half=None):
        x, y = (p, q) if colour == 0 else (q, p)
        r, c = self.sub(colour, half)
        return ref.at[x, y, pl.ds(*r), pl.ds(*c)]

    def whole_shape(self):
        if self.kind == "row":
            return (RING, RING, 2, self.rows, self.columns)
        return (RING, RING, self.rows, 2 * self.columns)


def remote(src, dst, sems, k, device):
    send, recv = sems
    return pltpu.make_async_remote_copy(
        src_ref=src, dst_ref=dst, send_sem=send.at[k], recv_sem=recv.at[k], device_id=device, device_id_type=MESH
    )


class Gather:
    N = 48

    def __init__(self, piece):
        self.piece = piece

    def scratch(self):
        return [pltpu.SemaphoreType.DMA((self.N,)), pltpu.SemaphoreType.DMA((self.N,)), pltpu.SemaphoreType.DMA]

    def bind(self, own, whole, send, recv, local):
        self.own, self.whole, self.sems, self.local = own, whole, (send, recv), local
        return self

    def copies(self, here):
        piece, own, whole, core = self.piece, self.own, self.whole, here.core
        out = {}

        def of_colour(colour):
            p, q = here.pq(colour)
            p1, pm, q1, qm = ahead(p, 1), ahead(p, RING - 1), ahead(q, 1), ahead(q, RING - 1)
            p2, q2 = ahead(p, 2), ahead(q, 2)
            at = functools.partial(piece.of_whole, whole, core, colour)
            dev = functools.partial(here.device, colour)
            base = 24 * colour

            def add(name, k, src, dst, device):
                out[name, colour] = lambda: remote(src(), dst(), self.sems, base + k, device)

            mine = lambda: piece.of_own(own, colour)
            add("s1+", 0, mine, lambda: at(p, q), dev(p1, q))
            add("s1-", 1, mine, lambda: at(p, q), dev(pm, q))
            add("s2+", 2, lambda: at(pm, q, 0), lambda: at(pm, q, 0), dev(p1, q))
            add("s2-", 3, lambda: at(p1, q, 1), lambda: at(p1, q, 1), dev(pm, q))
            for k, (name, of) in enumerate((("own", p), ("before", pm), ("after", p1), ("far", p2))):
                src = mine if k == 0 else lambda of=of: at(of, q)
                add(f"{name}+", 4 + 4 * k, src, lambda of=of: at(of, q), dev(p, q1))
                add(f"{name}-", 5 + 4 * k, src, lambda of=of: at(of, q), dev(p, qm))
                add(f"{name} on+", 6 + 4 * k, lambda of=of: at(of, qm, 0), lambda of=of: at(of, qm, 0), dev(p, q1))
                add(f"{name} on-", 7 + 4 * k, lambda of=of: at(of, q1, 1), lambda of=of: at(of, q1, 1), dev(p, qm))
            for k, of in enumerate((q, qm, q1, q2)):
                add(f"d{k}", 20 + k, lambda of=of: at(ALL, of), lambda of=of: at(ALL, of), here.peer())

        of_colour(0)
        of_colour(1)
        return out

    def run(self, stage):
        here = Place()
        c = self.copies(here)
        both = lambda names, do: [do(c[name, colour]()) for name in names for colour in (0, 1)]
        start = lambda *names: both(names, lambda d: d.start())
        arrived = lambda *names: both(names, lambda d: d.wait_recv())
        local = lambda: pltpu.make_async_copy(
            self.own, self.piece.chip_of_core(self.whole, here.core, here.x, here.y), self.local
        )
        if stage == 0:
            start("s1+", "s1-", "own+", "own-")
            local().start()
        elif stage == 1:
            for name, then in (("s1+", "s2+"), ("s1-", "s2-")):
                arrived(name)
                start(then)
            start("before+", "before-", "after+", "after-")
        elif stage == 2:
            for name in ("own+", "own-"):
                arrived(name)
                start(f"{name[:-1]} on{name[-1]}")
            arrived("s2+", "s2-")
            start("far+", "far-")
            local().wait()
            start("d0")
        elif stage == 3:
            for name in ("before+", "before-", "after+", "after-"):
                arrived(name)
                start(f"{name[:-1]} on{name[-1]}")
        elif stage == 4:
            for name, peer in (("far+", "d1"), ("far-", "d2")):
                arrived(name)
                start(f"{name[:-1]} on{name[-1]}", peer)
        else:
            arrived(*(f"{name} on{way}" for name in ("own", "before", "after", "far") for way in "+-"))
            start("d3")
            arrived("d0", "d1", "d2", "d3")
            both([n for n, colour in c if colour == 0], lambda d: d.wait_send())


class Scatter:
    def __init__(self, piece, which):
        self.piece, self.which = piece, which

    def scratch(self):
        piece = self.piece
        full = (RING, RING, piece.rows, piece.columns)
        c, h0, h1 = piece.shape(0, None), piece.shape(0, 0), piece.shape(0, 1)
        vm = lambda *shape, dtype=BF16: pltpu.VMEM(shape, dtype)
        per = [
            vm(2, RING, *h0), vm(2, RING, *h1), vm(2, RING, *c), vm(2, RING, *c),
            vm(2, *h0), vm(2, *h1), vm(2, *c), vm(2, *c),
            vm(2, RING, *c, dtype=F32),
        ]
        return [
            vm(*full), vm(*full), *per,
            pltpu.SemaphoreType.DMA((17,)), pltpu.SemaphoreType.DMA((17,)), pltpu.SemaphoreType.DMA,
        ]

    def bind(self, terms, result, *scratch):
        self.terms, self.result = terms if self.which is None else terms.at[self.which], result
        self.t, self.r, *self.landing, self.acc, send, recv, self.local = scratch
        self.sems = (send, recv)
        return self

    def copies(self, here):
        piece, t = self.piece, self.t
        far_a, far_b, near_a, near_b, last_far_a, last_far_b, last_near_a, last_near_b = self.landing
        out = {}

        def of_colour(colour):
            p, q = here.pq(colour)
            p1, pm, p2 = ahead(p, 1), ahead(p, RING - 1), ahead(p, 2)
            q1, qm, q2 = ahead(q, 1), ahead(q, RING - 1), ahead(q, 2)
            at = functools.partial(piece.of_pieces, t, colour)
            dev = functools.partial(here.device, colour)
            base = 8 * colour

            def add(name, k, src, dst, device):
                out[name, colour] = lambda: remote(src(), dst.at[colour], self.sems, base + k, device)

            add("F+", 0, lambda: at(ALL, q2, 0), far_a, dev(p, q1))
            add("F-", 1, lambda: at(ALL, q2, 1), far_b, dev(p, qm))
            add("N+", 2, lambda: at(ALL, q1), near_a, dev(p, q1))
            add("N-", 3, lambda: at(ALL, qm), near_b, dev(p, qm))
            add("f+", 4, lambda: at(p2, q, 0), last_far_a, dev(p1, q))
            add("f-", 5, lambda: at(p2, q, 1), last_far_b, dev(pm, q))
            add("n+", 6, lambda: at(p1, q), last_near_a, dev(p1, q))
            add("n-", 7, lambda: at(pm, q), last_near_b, dev(pm, q))

        of_colour(0)
        of_colour(1)
        return out

    def run(self, stage):
        here = Place()
        piece, t, r, acc = self.piece, self.t, self.r, self.acc
        far_a, far_b, near_a, near_b, last_far_a, last_far_b, last_near_a, last_near_b = self.landing
        c = self.copies(here)
        both = lambda names, do: [do(c[name, colour]()) for name in names for colour in (0, 1)]
        arrived = lambda *names: both(names, lambda d: d.wait_recv())
        peer = lambda: remote(piece.all_of_core(self.terms, 1 - here.core), r, self.sems, 16, here.peer())
        local = lambda: pltpu.make_async_copy(piece.all_of_core(self.terms, here.core), t, self.local)
        wide = lambda ref: ref[...].astype(F32)
        if stage == 0:
            peer().start()
            local().start()
            return
        if stage == 1:
            local().wait()
            peer().wait_recv()
        if stage == 2:
            arrived("F+", "F-")
        if stage == 3:
            arrived("N+", "N-")
        if stage == 4:
            arrived("f+", "f-")
        if stage == 5:
            arrived("n+", "n-")
        for colour in (0, 1):
            p, q = here.pq(colour)
            p1, pm, p2 = ahead(p, 1), ahead(p, RING - 1), ahead(p, 2)
            q1, qm, q2 = ahead(q, 1), ahead(q, RING - 1), ahead(q, 2)
            own = lambda pp, qq, half=None: wide(piece.of_pieces(t, colour, pp, qq, half)) + wide(
                piece.of_pieces(r, colour, pp, qq, half)
            )

            def put(pp, qq, value, half=None):
                piece.of_pieces(t, colour, pp, qq, half)[...] = value.astype(BF16)

            h0, h1 = piece.inside(0), piece.inside(1)
            if stage == 1:
                for i in range(RING):
                    put(i, q2, own(i, q2))
                c["F+", colour]().start()
                c["F-", colour]().start()
            elif stage == 2:
                for i in range(RING):
                    put(i, q1, own(i, q1, 0) + far_a[colour, i].astype(F32), 0)
                    put(i, q1, own(i, q1, 1), 1)
                c["N+", colour]().start()
                for i in range(RING):
                    put(i, qm, own(i, qm, 0), 0)
                    put(i, qm, own(i, qm, 1) + far_b[colour, i].astype(F32), 1)
                c["N-", colour]().start()
            elif stage == 3:
                for i in range(RING):
                    acc[colour, i] = own(i, q) + near_a[colour, i].astype(F32) + near_b[colour, i].astype(F32)
                put(p2, q, acc[colour, p2])
                c["f+", colour]().start()
                c["f-", colour]().start()
            elif stage == 4:
                put(p1, q, acc[colour, p1, :, h0] + last_far_a[colour].astype(F32), 0)
                put(p1, q, acc[colour, p1, :, h1], 1)
                c["n+", colour]().start()
                put(pm, q, acc[colour, pm, :, h0], 0)
                put(pm, q, acc[colour, pm, :, h1] + last_far_b[colour].astype(F32), 1)
                c["n-", colour]().start()
            else:
                total = acc[colour, p] + last_near_a[colour].astype(F32) + last_near_b[colour].astype(F32)
                piece.of_own(self.result, colour)[...] = total.astype(BF16)
        if stage == 5:
            peer().wait_send()
            both([n for n, colour in c if colour == 0], lambda d: d.wait_send())


class Resident:
    def __init__(self, array, axis, size, outer=1):
        self.array, self.axis, self.outer = array, axis, outer
        self.parts = chunks(array.shape[axis], size)

    def scratch(self):
        return [pltpu.VMEM(self.array.shape, self.array.dtype), pltpu.SemaphoreType.DMA((self.outer * len(self.parts),))]

    def bind(self, hbm, vmem, sems):
        self.hbm, self.vmem, self.sems = hbm, vmem, sems
        return self

    def copy(self, w, j):
        index = [ALL] * len(self.array.shape)
        index[self.axis] = pl.ds(*self.parts[j])
        if self.outer > 1:
            index[0] = w
        index = tuple(index)
        return pltpu.make_async_copy(self.hbm.at[index], self.vmem.at[index], self.sems.at[w * len(self.parts) + j])


def kernel_call(name, grid, compute, inputs, outputs, resident=(), parts=1, gathers=(), scatters=(), at=None, collective_id=None):
    comms = [Gather(p) for p, _ in gathers] + [Scatter(p, w) for p, _, w in scatters]
    n_in, n_out = len(inputs), len(outputs)
    steps = math.prod(grid)
    any_space = pl.BlockSpec(memory_space=pltpu.HBM)
    in_vmem = lambda shape: pl.BlockSpec(shape, lambda *_: (0,) * len(shape), pipeline_mode=pl.Buffered(1))

    def spec(block, index):
        if index is None:
            return in_vmem(block)
        return pl.BlockSpec(block, index)

    in_specs = [spec(b, i) for _, b, i in inputs] + [any_space] * len(resident)
    out_specs = [spec(b, i) for *_, b, i in outputs]
    out_shape = [jax.ShapeDtypeStruct(s, d) for s, d, *_ in outputs]
    args = [a for a, *_ in inputs] + [r.array for r in resident]
    for piece, own in gathers:
        args.append(own)
        in_specs.append(in_vmem(own.shape))
        out_shape.append(jax.ShapeDtypeStruct(piece.whole_shape(), BF16))
        out_specs.append(any_space)
    for piece, terms, _ in scatters:
        args.append(terms)
        in_specs.append(any_space)
        shape = (piece.rows, piece.columns)
        out_shape.append(jax.ShapeDtypeStruct(shape, BF16))
        out_specs.append(in_vmem(shape))
    held = [r.scratch() for r in resident]
    comm_scratch = [c.scratch() for c in comms]
    scratch_shapes = [s for group in held + comm_scratch for s in group]
    last = steps * parts
    at = at or tuple(k * last // 6 for k in range(6))

    def body(*refs):
        refs = list(refs)
        take = lambda n: [refs.pop(0) for _ in range(n)]
        ins, res_in, comm_in = take(n_in), take(len(resident)), take(len(comms))
        outs, comm_out = take(n_out), take(len(comms))
        for r, i in zip(resident, res_in):
            r.bind(i, *take(2))
        for comm, i, o, s in zip(comms, comm_in, comm_out, comm_scratch):
            comm.bind(i, o, *take(len(s)))
        step = pl.program_id(0)
        for d in range(1, len(grid)):
            step = step * grid[d] + pl.program_id(d)

        if resident:
            @pl.when(step == 0)
            def _():
                for w in range(max(r.outer for r in resident)):
                    for j in range(max(len(r.parts) for r in resident)):
                        for r in resident:
                            if w < r.outer and j < len(r.parts):
                                r.copy(w, j).start()

        def act(slot):
            if slot == 0:
                greet()
            for k in range(6):
                if at[k] == slot:
                    for comm in comms:
                        comm.run(k)

        def hook(part):
            if comms:
                for slot in sorted({0, *at}):
                    if slot < last and slot % parts == part:
                        pl.when(step == slot // parts)(functools.partial(act, slot))

        def ready(j, *which):
            for r in which:
                for w in range(r.outer):
                    pl.when(step == w * (steps // r.outer))(lambda: r.copy(w, j).wait())

        compute(hook, ready, ins, outs)
        if comms and any(a == last for a in at):
            pl.when(step == steps - 1)(functools.partial(act, last))

    params = dict(vmem_limit_bytes=VMEM_LIMIT, dimension_semantics=("arbitrary",) * len(grid))
    if comms:
        params |= dict(collective_id=collective_id, has_side_effects=True)
    return pl.pallas_call(
        body, grid=grid, in_specs=in_specs, out_specs=out_specs, out_shape=out_shape, scratch_shapes=scratch_shapes,
        compiler_params=pltpu.CompilerParams(**params), name=name,
    )(*args)


def dot(a, b, ca=1, cb=0):
    return lax.dot_general(a, b, (((ca,), (cb,)), ((), ())), preferred_element_type=F32)


def chunks(n, size=None):
    size = size or CHUNK
    return [(i, min(size, n - i)) for i in range(0, n, size)]


def normed(h):
    wide = h.astype(F32)
    scale = lax.rsqrt(jnp.mean(wide**2, -1, keepdims=True) + EPS)
    return (wide * scale).astype(BF16)


def norm_back(h, da, dy):
    wide, da = h.astype(F32), da.astype(F32)
    scale = lax.rsqrt(jnp.mean(wide**2, -1, keepdims=True) + EPS)
    by_scale = jnp.sum(da * wide, -1, keepdims=True)
    by_mean = by_scale * (-0.5) * scale * scale * scale
    return dy + (da * scale + wide * (by_mean * (2.0 / h.shape[-1]))).astype(BF16)


def gated(g, u):
    s = jax.nn.sigmoid(g)
    return (g * s * u).astype(BF16)


def gated_back(g, u, dh):
    s = jax.nn.sigmoid(g)
    silu = g * s
    return ((dh * u) * (s + silu * (1.0 - s))).astype(BF16), (dh * silu).astype(BF16)


def rows_of(array, bm=None):
    bm = bm or BM
    block = (bm, *array.shape[1:])
    return array, block, lambda i: (i, 0)


def whole(array):
    return array, array.shape, None


def k_norm(x, **comm):
    t, d = x.shape

    def compute(hook, ready, ins, outs):
        hook(0)
        outs[0][...] = normed(ins[0][...])

    bm = t // 8
    return kernel_call("norm", (8,), compute, [rows_of(x, bm)], [((t, d), BF16, (bm, d), lambda i: (i, 0))], **comm)


def k_gate_up(a, wg, wu, **comm):
    t, f = a.shape[0], wg.shape[1]
    wg, wu = Resident(wg, 1, f), Resident(wu, 1, f)

    def compute(hook, ready, ins, outs):
        g_out, u_out, h_out = outs
        x = ins[0][...]
        hook(0)
        ready(0, wg)
        g_out[...] = dot(x, wg.vmem[...])
        hook(1)
        ready(0, wu)
        u = dot(x, wu.vmem[...])
        u_out[...] = u
        h_out[...] = gated(g_out[...], u)

    o = lambda dt: ((t, f), dt, (BM, f), lambda i: (i, 0))
    return kernel_call(
        "gate_up", (t // BM,), compute, [rows_of(a)], [o(F32), o(F32), o(BF16)], resident=[wg, wu], parts=2, **comm
    )


def k_middle(a, dy, wg, wu, wd):
    t, f = a.shape[0], wg.shape[1]

    def compute(hook, ready, ins, outs):
        a, dy, wg, wu, wd = ins
        dgu, h_out = outs
        x, dy = a[...], dy[...]
        for lo, n in chunks(f, 512):
            cols = pl.ds(lo, n)
            g, u = dot(x, wg[:, cols]), dot(x, wu[:, cols])
            dh = dot(dy, wd[cols, :], 1, 1).astype(BF16).astype(F32)
            h_out[:, cols] = gated(g, u)
            dgu[0, :, cols], dgu[1, :, cols] = gated_back(g, u, dh)

    return kernel_call(
        "middle", (t // BM,), compute, [rows_of(a), rows_of(dy), whole(wg), whole(wu), whole(wd)],
        [((2, t, f), BF16, (2, BM, f), lambda i: (0, i, 0)), ((t, f), BF16, (BM, f), lambda i: (i, 0))],
    )


def k_down(h, x, wd, **comm):
    t, d = x.shape

    def compute(hook, ready, ins, outs):
        h, x, wd = ins
        hook(0)
        y = x[...] + dot(h[...], wd[...]).astype(BF16)
        outs[0][...] = y
        outs[1][...] = normed(y)

    o = ((t, d), BF16, (BM, d), lambda i: (i, 0))
    return kernel_call("down", (t // BM,), compute, [rows_of(h), rows_of(x), whole(wd)], [o, o], **comm)


def k_hidden_back(dy, g, u, wd, **comm):
    t, f = g.shape
    wd = Resident(wd, 0, CHUNK)

    def compute(hook, ready, ins, outs):
        dy, g, u = ins
        (dgu,) = outs
        x = dy[...]
        for j, (lo, n) in enumerate(chunks(f)):
            hook(j)
            ready(j, wd)
            cols = pl.ds(lo, n)
            dh = dot(x, wd.vmem[cols, :], 1, 1).astype(BF16).astype(F32)
            dgu[0, :, cols], dgu[1, :, cols] = gated_back(g[:, cols], u[:, cols], dh)

    return kernel_call(
        "hidden_back", (t // BM,), compute, [rows_of(dy), rows_of(g), rows_of(u)],
        [((2, t, f), BF16, (2, BM, f), lambda i: (0, i, 0))], resident=[wd], parts=len(wd.parts), **comm,
    )


def k_grad_down(h, dy, **comm):
    (t, f), d = h.shape, dy.shape[1]
    bn = f // 5

    def compute(hook, ready, ins, outs):
        hook(0)
        outs[0][...] = dot(ins[0][...], ins[1][...], 0, 0).astype(BF16)

    return kernel_call(
        "grad_down", (5,), compute, [(h, (t, bn), lambda i: (0, i)), whole(dy)],
        [((f, d), BF16, (bn, d), lambda i: (i, 0))], **comm,
    )


def k_grad_gate_up(a, dgu, **comm):
    (t, d), f = a.shape, dgu.shape[2]
    bm = GRAD_ROWS
    dgu = Resident(dgu, 2, f, outer=2)

    def compute(hook, ready, ins, outs):
        x = ins[0][...]
        w = pl.program_id(0)
        for j, (lo, n) in enumerate(chunks(f, f)):
            hook(j)
            ready(j, dgu)
            cols = pl.ds(lo, n)
            outs[0][0, :, cols] = dot(x, dgu.vmem[w, :, cols], 0, 0).astype(BF16)

    return kernel_call(
        "grad_gate_up", (2, d // bm), compute, [(a, (t, bm), lambda w, i: (0, i))],
        [((2, d, f), BF16, (1, bm, f), lambda w, i: (w, i, 0))], resident=[dgu], parts=len(dgu.parts), **comm,
    )


def k_input_back(dgu, wg, wu, x, dy, **comm):
    t, d = x.shape
    f = dgu.shape[2]
    wg, wu = Resident(wg, 0, d), Resident(wu, 0, d)

    def compute(hook, ready, ins, outs):
        dgu, x, dy = ins
        hook(0)
        ready(0, wg)
        by_g = dot(dgu[0], wg.vmem[...], 1, 1).astype(BF16)
        hook(1)
        ready(0, wu)
        da = by_g + dot(dgu[1], wu.vmem[...], 1, 1).astype(BF16)
        outs[0][...] = norm_back(x[...], da, dy[...])

    return kernel_call(
        "input_back", (t // BM,), compute, [(dgu, (2, BM, f), lambda i: (0, i, 0)), rows_of(x), rows_of(dy)],
        [((t, d), BF16, (BM, d), lambda i: (i, 0))], resident=[wg, wu], parts=2, **comm,
    )


def solution(mesh):
    members = mesh.shape["dp"]
    swap = [(i, i ^ 1) for i in range(members)]

    def step(x, dy, w_gate, w_up, w_down):
        x, dy = x[0], dy[0]
        core = lax.rem(lax.axis_index("dp"), 2)
        rows, f = w_gate.shape[1:]
        deep, d = w_down.shape[1:]
        half = d // 2
        row, col = Piece("row", rows, f), Piece("col", 2 * deep, half)
        square = lambda w: w.reshape(-1, w.shape[-1])

        keep = lax.dynamic_slice_in_dim(w_down, core * half, half, 2)
        other = lax.ppermute(lax.dynamic_slice_in_dim(w_down, (1 - core) * half, half, 2), "dp", swap)
        down = jnp.where(core == 0, jnp.concatenate([keep, other], 1), jnp.concatenate([other, keep], 1))

        a0, wg0, wu0 = k_norm(x, gathers=[(row, w_gate[0]), (row, w_up[0])], at=(0, 4, 5, 6, 7, 8), collective_id=0)
        wg0, wu0 = square(wg0), square(wu0)
        g0, u0, h0, wd0, wg1 = k_gate_up(
            a0, wg0, wu0, gathers=[(col, down[0]), (row, w_gate[1])], at=(0, 3, 6, 10, 13, 16), collective_id=1
        )
        wd0, wg1 = square(wd0), square(wg1)
        x1, a1, wu1, wd1 = k_down(
            h0, x, wd0, gathers=[(row, w_up[1]), (col, down[1])], at=(0, 3, 5, 8, 8, 8), collective_id=2
        )
        wu1, wd1 = square(wu1), square(wd1)

        as_row = lambda g: g.reshape(2, RING, RING, 2, rows, f)
        as_col = lambda g: g.reshape(RING, RING, 2 * deep, d)
        dgu1, h1 = k_middle(a1, dy, wg1, wu1, wd1)
        (gd1,) = k_grad_down(h1, dy)
        ggu1, by_d1 = k_grad_gate_up(a1, dgu1, scatters=[(col, as_col(gd1), None)], at=(0, 2, 4, 7, 8, 8), collective_id=3)
        dx1, by_g1 = k_input_back(
            dgu1, wg1, wu1, x1, dy, scatters=[(row, as_row(ggu1), 0)], at=(0, 4, 8, 13, 15, 16), collective_id=4
        )
        (gd0,) = k_grad_down(h0, dx1)
        dgu0, by_u1 = k_hidden_back(
            dx1, g0, u0, wd0, scatters=[(row, as_row(ggu1), 1)], at=(0, 7, 15, 27, 31, 32), collective_id=5
        )
        ggu0, by_d0 = k_grad_gate_up(a0, dgu0, scatters=[(col, as_col(gd0), None)], at=(0, 2, 4, 7, 8, 8), collective_id=6)
        by_x, by_g0, by_u0 = k_input_back(
            dgu0, wg0, wu0, x, dx1, scatters=[(row, as_row(ggu0), 0), (row, as_row(ggu0), 1)],
            at=(0, 5, 10, 16, 16, 16), collective_id=7,
        )

        by_down = jnp.stack([by_d0, by_d1])
        mine = lax.dynamic_slice_in_dim(by_down, core * deep, deep, 1)
        theirs = lax.ppermute(lax.dynamic_slice_in_dim(by_down, (1 - core) * deep, deep, 1), "dp", swap)
        by_down = jnp.where(core == 0, jnp.concatenate([mine, theirs], 2), jnp.concatenate([theirs, mine], 2))
        return by_x[None], jnp.stack([by_g0, by_g1]), jnp.stack([by_u0, by_u1]), by_down

    tokens, weights, grads = P(("rep", "dp")), P(None, "dp"), P("rep", "dp")
    return jax.shard_map(
        step, mesh=mesh, in_specs=(tokens, tokens, weights, weights, weights), out_specs=(tokens, grads, grads, grads),
        check_vma=False,
    )
```
